32 devices in a mesh: tm: 4 (over z), mp: 4 (over y, x), dec: 2 (over core).
Axes of the slice: x: 2, y: 2, z: 4, core: 2. Of those that a mesh axis runs over, the one named last changes fastest.
Arguments:
- latents: bfloat16 [1024, 3072], P('tm'), may hold values from -6 to 6
- modulation: float32 [4, 3, 3072], P('tm'), may hold values from -1.5 to 3.5
- w_qkv: bfloat16 [3, 3072, 3072], P(None, None, ('mp', 'dec'))
- w_out: bfloat16 [3072, 3072], P(('mp', 'dec')), may hold values from -0.109375 to 0.109375
- block_mask: int32 [4, 4], replicated, may hold values from 0 to 1, as said below
- lengths: int32 [4], replicated, may hold values from 64 to 256, as said below
Outputs:
- updated: bfloat16 [1024, 3072], P('tm', ('mp', 'dec'))
The draws below stay inside these ranges and needn't reach their ends.
Inputs may be any that keep to these rules, and one draw needn't show every extreme that they name: block_mask[i, i] = 1 and block_mask[i, j] = 0 for j > i. `lengths`: some group of index 2 or more has all 256 tokens live.
All inputs are finite; a program needn't handle non-finite values.
Results may differ from the reference program's by a relative error of at most 0.0057.
Values may be sent and summed in bfloat16 or wider, within the bound.
A program may use at most 192 MiB of HBM per device.

```python
import jax
import jax.numpy as jnp
from jax import lax

D = 3072
HEADS = 24
HS = 128
TOK = 256
GROUPS = 4
TOKENS = 1024
N_TM = 4


def causal_pattern(key):
    coins = jax.random.randint(key, (GROUPS, GROUPS), 0, 5) > 0
    rows_index = jnp.arange(GROUPS, dtype=jnp.int32)[:, None]
    cols_index = jnp.arange(GROUPS, dtype=jnp.int32)[None, :]
    below = jnp.where(coins, 1, 0).astype(jnp.int32)
    return jnp.where(rows_index == cols_index, 1, jnp.where(cols_index < rows_index, below, 0)).astype(jnp.int32)


def full_group(key):
    second = jax.random.fold_in(key, 1)
    return jax.random.randint(second, (), GROUPS // 2, GROUPS).astype(jnp.int32)


def draw_modulation(key, part):
    first = jax.random.fold_in(key, 0)
    base = jnp.clip(0.5 * jax.random.normal(first, (GROUPS, 3, D), jnp.float32), -1.5, 1.5)
    return base


def draw_w_qkv(key, part):
    first = jax.random.fold_in(key, 0)
    scale = D ** (-0.5)
    weights = jnp.clip(jax.random.normal(first, (3, D, HEADS * HS), jnp.float32), -4.0, 4.0) * scale
    return weights.astype(jnp.bfloat16)


def draw_block_mask(key, part):
    return causal_pattern(key)


def draw_lengths(key, part):
    first = jax.random.fold_in(key, 0)
    drawn = jax.random.randint(first, (GROUPS,), TOK // 4, TOK + 1)
    target = full_group(key)
    return drawn.at[target].set(TOK).astype(jnp.int32)


def block_levels(key, dims, shards, smallest, top_value):
    level, own = 1.0, jax.random.fold_in(key, 6)
    for axis_at, shards_of in shards:
        draws = jnp.exp(jax.random.uniform(jax.random.fold_in(own, axis_at), (shards_of,), jnp.float32, smallest / len(shards), top_value / len(shards)))
        level = level * jnp.repeat(draws, dims[axis_at] // shards_of).reshape([-1 if axis == axis_at else 1 for axis in range(len(dims))])
    return level


def gaussian(rng, dims, scale, bound, pieces=(), held_as=jnp.bfloat16):
    loudness = block_levels(rng, dims, pieces, -0.22, 0.18) if pieces else 1.0
    array = jax.random.normal(rng, dims, jnp.float32) * scale * loudness
    return jnp.minimum(jnp.maximum(array, -bound), bound).astype(held_as)


def setup_inputs(seed: int = 0) -> dict:
    streams_of = jax.random.split(jax.random.key(seed), 7)
    latents = gaussian(streams_of[0], (TOKENS, D), 1.0, 6.0, ((0, 4),))
    modulation = draw_modulation(jax.random.fold_in(streams_of[6], 71), 0)
    w_qkv = draw_w_qkv(jax.random.fold_in(streams_of[6], 71), 0)
    w_out = gaussian(streams_of[3], (HEADS * HS, D), (HEADS * HS) ** -0.5, 0.109375, ((0, 8),))
    block_mask = draw_block_mask(jax.random.fold_in(streams_of[6], 71), 0)
    lengths = draw_lengths(jax.random.fold_in(streams_of[6], 71), 0)
    return dict(latents=latents, modulation=modulation, w_qkv=w_qkv, w_out=w_out, block_mask=block_mask, lengths=lengths)


def reference(latents, modulation, w_qkv, w_out, block_mask, lengths):
    wide = latents.astype(jnp.float32)
    mean = lax.optimization_barrier(jnp.mean(wide, axis=-1, keepdims=True))
    var = lax.optimization_barrier(jnp.mean((wide - mean) ** 2, axis=-1, keepdims=True))
    normed = (wide - mean) * lax.rsqrt(var + 1e-06)
    per_token = jnp.repeat(modulation, TOK, axis=0)
    adapted = (normed * (1.0 + per_token[:, 1]) + per_token[:, 0]).astype(jnp.bfloat16)
    query = jnp.dot(adapted, w_qkv[0], preferred_element_type=jnp.float32).astype(jnp.bfloat16)
    key = jnp.dot(adapted, w_qkv[1], preferred_element_type=jnp.float32).astype(jnp.bfloat16)
    value = jnp.dot(adapted, w_qkv[2], preferred_element_type=jnp.float32).astype(jnp.bfloat16)
    slots = jnp.arange(TOKENS, dtype=jnp.int32)
    key_group = slots // TOK
    key_live = slots % TOK < lengths[key_group]
    key_all = key.astype(jnp.float32).reshape(TOKENS, HEADS, HS)
    value_all = value.astype(jnp.float32).reshape(TOKENS, HEADS, HS)

    def one_group(group):
        rows = lax.dynamic_slice_in_dim(query, group * TOK, TOK, 0)
        rows = rows.astype(jnp.float32).reshape(TOK, HEADS, HS)
        score = jnp.einsum('thd,shd->hts', rows, key_all) / jnp.sqrt(jnp.float32(HS))
        allowed = (block_mask[group][key_group] == 1) & key_live
        score = jnp.where(allowed[None, None, :], score, jnp.float32(-1e+30))
        peak = lax.optimization_barrier(jnp.max(score, axis=-1, keepdims=True))
        weight = jnp.exp(score - peak) * allowed[None, None, :].astype(jnp.float32)
        total = lax.optimization_barrier(jnp.sum(weight, axis=-1))
        weight_b = lax.optimization_barrier(weight.astype(jnp.bfloat16)).astype(jnp.float32)
        mixed = jnp.einsum('hts,shd->thd', weight_b, value_all)
        mixed = mixed / jnp.transpose(total)[:, :, None]
        return mixed.reshape(TOK, HEADS * HS).astype(jnp.bfloat16)
    attended = lax.map(one_group, jnp.arange(N_TM, dtype=jnp.int32)).reshape(TOKENS, HEADS * HS)
    branch = jnp.dot(attended, w_out, preferred_element_type=jnp.float32)
    return (wide + per_token[:, 2] * branch).astype(jnp.bfloat16)
```

```python
import functools
import math

import jax
import jax.numpy as jnp
from jax import lax
from jax.experimental import pallas as pl
from jax.experimental.pallas import tpu as pltpu
from jax.sharding import PartitionSpec as P

HS = 128
EPS = 1e-6
MESH = pl.DeviceIdType.MESH
F32 = jnp.float32
BF16 = jnp.bfloat16


def kernel(
    sizes,
    lat_hbm,
    mod_ref,
    wqkv_hbm,
    wout_hbm,
    mask_ref,
    len_ref,
    out_ref,
    x,
    adapted,
    w,
    wo,
    q,
    kv,
    peak,
    total,
    accum,
    attended,
    tx1,
    rx1,
    tx2,
    rx2,
    x_sem,
    w_sem,
    wo_sem,
    kv_send,
    kv_recv,
    send1,
    recv1,
    send2,
    recv2,
):
    n, M, D, parts = sizes
    tok, width = x.shape
    columns = q.shape[1]
    heads = columns // HS
    share = out_ref.shape[1]
    depth = width // parts
    mine = lax.axis_index("tm")
    mp = lax.axis_index("mp")
    dec = lax.axis_index("dec")

    def load_w(which, place, part):
        rows = pl.ds(part * depth, depth)
        return pltpu.make_async_copy(
            wqkv_hbm.at[which, rows],
            w.at[rows, pl.ds(place * columns, columns)],
            w_sem.at[place, part],
        )

    load_x = pltpu.make_async_copy(lat_hbm, x, x_sem)
    load_wo = pltpu.make_async_copy(wout_hbm, wo, wo_sem)
    load_x.start()
    for part in range(parts):
        load_w(1, 0, part).start()
        load_w(2, 1, part).start()
    for part in range(parts):
        load_w(0, 2, part).start()
    load_wo.start()

    barrier = pltpu.get_barrier_semaphore()
    right = lax.rem(mine + 1, n)
    left = lax.rem(mine + n - 1, n)
    for other in (left, right):
        pl.semaphore_signal(barrier, inc=1, device_id={"tm": other}, device_id_type=MESH)
    for j in range(1, M):
        pl.semaphore_signal(
            barrier, inc=1, device_id={"mp": lax.rem(mp + j, M)}, device_id_type=MESH
        )
    for d in range(1, D):
        pl.semaphore_signal(
            barrier, inc=1, device_id={"dec": lax.rem(dec + d, D)}, device_id_type=MESH
        )

    load_x.wait()
    shift = mod_ref[0, 0:1, :]
    scale = 1.0 + mod_ref[0, 1:2, :]
    step = 16

    def norm(i, carry):
        rows = pl.ds(pl.multiple_of(i * step, step), step)
        wide = x[rows, :].astype(F32)
        mean = jnp.sum(wide, axis=-1, keepdims=True) * (1.0 / width)
        centred = wide - mean
        var = jnp.sum(centred * centred, axis=-1, keepdims=True) * (1.0 / width)
        adapted[rows, :] = (centred * lax.rsqrt(var + EPS) * scale + shift).astype(BF16)
        return carry

    lax.fori_loop(0, tok // step, norm, 0)

    def project(first, count):
        out = None
        for part in range(parts):
            for place in range(first, first + count):
                load_w((1, 2, 0)[place], place, part).wait()
            rows = pl.ds(part * depth, depth)
            piece = jnp.dot(
                adapted[:, rows],
                w[rows, pl.ds(first * columns, count * columns)],
                preferred_element_type=F32,
            )
            out = piece if out is None else out + piece
        return out.astype(BF16)

    def pass_on(hop, head):
        return pltpu.make_async_remote_copy(
            src_ref=kv.at[hop - 1, head],
            dst_ref=kv.at[hop, head],
            send_sem=kv_send.at[hop - 1, head],
            recv_sem=kv_recv.at[hop - 1, head],
            device_id={"tm": right},
            device_id_type=MESH,
        )

    own = project(0, 2)
    for head in range(heads):
        kv[0, head, 0] = own[:, head * HS : (head + 1) * HS]
        kv[0, head, 1] = own[:, columns + head * HS : columns + (head + 1) * HS]
    pl.semaphore_wait(barrier, 2 + (M - 1) + (D - 1))

    @pl.when(mine + 1 < n)
    def _():
        for head in range(heads):
            pass_on(1, head).start()

    q[...] = project(2, 1)
    slots = lax.broadcasted_iota(jnp.int32, (1, tok), 1)
    factor = math.log2(math.e) / math.sqrt(HS)

    def scores(hop, head):
        group = mine - hop
        live = jnp.where(mask_ref[mine, group] == 1, len_ref[group], 0)
        score = lax.dot_general(
            q[:, head * HS : (head + 1) * HS],
            kv[hop, head, 0],
            (((1,), (1,)), ((), ())),
            preferred_element_type=F32,
        )
        return jnp.where(slots < live, score * factor, -1e30)

    for head in range(heads):
        score = scores(0, head)
        top = jnp.max(score, axis=-1, keepdims=True)
        weight = jnp.exp2(score - top)
        peak[head] = top
        total[head] = jnp.sum(weight, axis=-1, keepdims=True)
        accum[head] = jnp.dot(
            weight.astype(BF16), kv[0, head, 1], preferred_element_type=F32
        )

    def hop_step(hop, carry):
        @pl.when(mine >= hop)
        def _():
            for head in range(heads):
                pass_on(hop, head).wait_recv()

                @pl.when((mine + 1 < n) & (hop + 1 < n))
                def _():
                    pass_on(hop + 1, head).start()

                score = scores(hop, head)
                old = peak[head]
                top = jnp.maximum(old, jnp.max(score, axis=-1, keepdims=True))
                keep = jnp.exp2(old - top)
                weight = jnp.exp2(score - top)
                peak[head] = top
                total[head] = total[head] * keep + jnp.sum(weight, axis=-1, keepdims=True)
                accum[head] = accum[head] * keep + jnp.dot(
                    weight.astype(BF16), kv[hop, head, 1], preferred_element_type=F32
                )

        return carry

    lax.fori_loop(1, n, hop_step, 0)
    for head in range(heads):
        attended[:, head * HS : (head + 1) * HS] = (accum[head] / total[head]).astype(BF16)
    load_wo.wait()

    def term(chip, core):
        start = pl.multiple_of((chip * D + core) * share, share)
        return jnp.dot(attended[...], wo[:, pl.ds(start, share)], preferred_element_type=F32)

    def to_core(d, j):
        return pltpu.make_async_remote_copy(
            src_ref=tx1.at[d - 1, j],
            dst_ref=rx1.at[d - 1, j],
            send_sem=send1.at[d - 1, j],
            recv_sem=recv1.at[d - 1, j],
            device_id={"dec": lax.rem(dec + d, D)},
            device_id_type=MESH,
        )

    def to_chip(j):
        return pltpu.make_async_remote_copy(
            src_ref=tx2.at[j - 1],
            dst_ref=rx2.at[j - 1],
            send_sem=send2.at[j - 1],
            recv_sem=recv2.at[j - 1],
            device_id={"mp": lax.rem(mp + j, M)},
            device_id_type=MESH,
        )

    order = list(range(1, M)) + [0]
    for j in order:
        for d in range(1, D):
            tx1[d - 1, j] = term(lax.rem(mp + j, M), lax.rem(dec + d, D)).astype(BF16)
            to_core(d, j).start()
    for j in order:
        part = term(lax.rem(mp + j, M), dec)
        for d in range(1, D):
            to_core(d, j).wait_recv()
            part = part + rx1[d - 1, j].astype(F32)
        if j > 0:
            tx2[j - 1] = part.astype(BF16)
            to_chip(j).start()
    for j in range(1, M):
        to_chip(j).wait_recv()
        part = part + rx2[j - 1].astype(F32)
    mine_columns = pl.ds(pl.multiple_of((mp * D + dec) * share, share), share)
    gate = mod_ref[0, 2:3, mine_columns]
    out_ref[...] = (x[:, mine_columns].astype(F32) + gate * part).astype(BF16)

    for j in order:
        for d in range(1, D):
            to_core(d, j).wait_send()
    for j in range(1, M):
        to_chip(j).wait_send()

    def sent(hop, carry):
        @pl.when((mine + 1 < n) & (mine >= hop - 1))
        def _():
            for head in range(heads):
                pass_on(hop, head).wait_send()

        return carry

    lax.fori_loop(1, n, sent, 0)


def solution(mesh):
    n, M, D = mesh.shape["tm"], mesh.shape["mp"], mesh.shape["dec"]

    def shards(latents, modulation, w_qkv, w_out, block_mask, lengths):
        tok, width = latents.shape
        columns = w_qkv.shape[2]
        heads = columns // HS
        share = width // (M * D)
        parts = 3
        vmem = pl.BlockSpec(memory_space=pltpu.VMEM)
        smem = pl.BlockSpec(memory_space=pltpu.SMEM)
        anywhere = pl.BlockSpec(memory_space=pl.ANY)
        dma = pltpu.SemaphoreType.DMA
        return pl.pallas_call(
            functools.partial(kernel, (n, M, D, parts)),
            out_shape=jax.ShapeDtypeStruct((tok, share), BF16),
            in_specs=[anywhere, vmem, anywhere, anywhere, smem, smem],
            out_specs=vmem,
            scratch_shapes=[
                pltpu.VMEM((tok, width), BF16),
                pltpu.VMEM((tok, width), BF16),
                pltpu.VMEM((width, 3 * columns), BF16),
                pltpu.VMEM((columns, width), BF16),
                pltpu.VMEM((tok, columns), BF16),
                pltpu.VMEM((n, heads, 2, tok, HS), BF16),
                pltpu.VMEM((heads, tok, 1), F32),
                pltpu.VMEM((heads, tok, 1), F32),
                pltpu.VMEM((heads, tok, HS), F32),
                pltpu.VMEM((tok, columns), BF16),
                pltpu.VMEM((D - 1, M, tok, share), BF16),
                pltpu.VMEM((D - 1, M, tok, share), BF16),
                pltpu.VMEM((M - 1, tok, share), BF16),
                pltpu.VMEM((M - 1, tok, share), BF16),
                dma,
                dma((3, parts)),
                dma,
                dma((n - 1, heads)),
                dma((n - 1, heads)),
                dma((D - 1, M)),
                dma((D - 1, M)),
                dma((M - 1,)),
                dma((M - 1,)),
            ],
            compiler_params=pltpu.CompilerParams(collective_id=0, has_side_effects=True),
        )(latents, modulation, w_qkv, w_out, block_mask, lengths)

    return jax.shard_map(
        shards,
        mesh=mesh,
        in_specs=(
            P("tm", None),
            P("tm", None, None),
            P(None, None, ("mp", "dec")),
            P(("mp", "dec"), None),
            P(),
            P(),
        ),
        out_specs=P("tm", ("mp", "dec")),
        check_vma=False,
    )
```

```python
import functools
import math

import jax
import jax.numpy as jnp
from jax import lax
from jax.experimental import pallas as pl
from jax.experimental.pallas import tpu as pltpu
from jax.sharding import PartitionSpec as P

HS = 128
EPS = 1e-6
FAR_BYTES = 16 * 2**20
MESH = pl.DeviceIdType.MESH
F32 = jnp.float32
BF16 = jnp.bfloat16


def kernel(
    sizes,
    lat_hbm,
    mod_ref,
    wqkv_hbm,
    wout_hbm,
    mask_ref,
    len_ref,
    out_ref,
    x,
    adapted,
    w,
    wo,
    q,
    kv,
    peak,
    total,
    accum,
    attended,
    tx1,
    rx1,
    tx2,
    rx2,
    mods,
    far,
    x_sem,
    w_sem,
    wo_sem,
    kv_send,
    kv_recv,
    send1,
    recv1,
    send2,
    recv2,
    z_send,
    z_recv,
    xy_send,
    xy_recv,
    core_send,
    core_recv,
):
    n, M, D, parts, chunks, far_hops = sizes
    near = n - 1 - far_hops
    tok, width = x.shape
    columns = q.shape[1]
    heads = columns // HS
    share = out_ref.shape[1]
    depth = width // parts
    mine = lax.axis_index("tm")
    mp = lax.axis_index("mp")
    dec = lax.axis_index("dec")

    def load_w(which, place, part):
        rows = pl.ds(part * depth, depth)
        return pltpu.make_async_copy(
            wqkv_hbm.at[which, rows],
            w.at[rows, pl.ds(place * columns, columns)],
            w_sem.at[place, part],
        )

    pieces = M * D
    eighth = tok // pieces
    chunk = eighth // chunks
    place = mp * D + dec

    def load_x(i):
        rows = pl.ds(pl.multiple_of(i * eighth, eighth), eighth)
        return pltpu.make_async_copy(lat_hbm.at[rows], x.at[rows], x_sem.at[i])

    load_wo = pltpu.make_async_copy(wout_hbm, wo, wo_sem)
    for i in range(pieces):
        load_x(lax.rem(place + i, pieces)).start()
    for part in range(parts):
        load_w(1, 0, part).start()
        load_w(2, 1, part).start()
    for part in range(parts):
        load_w(0, 2, part).start()
    load_wo.start()

    barrier = pltpu.get_barrier_semaphore()
    right = lax.rem(mine + 1, n)
    left = lax.rem(mine + n - 1, n)
    others = [left, right]
    if far_hops:
        others += [lax.rem(mine + 2, n), lax.rem(mine + n - 2, n)]
    for other in others:
        pl.semaphore_signal(barrier, inc=1, device_id={"tm": other}, device_id_type=MESH)
    for j in range(1, M):
        pl.semaphore_signal(
            barrier, inc=1, device_id={"mp": lax.rem(mp + j, M)}, device_id_type=MESH
        )
    for d in range(1, D):
        pl.semaphore_signal(
            barrier, inc=1, device_id={"dec": lax.rem(dec + d, D)}, device_id_type=MESH
        )

    tiles = width // HS
    for i in range(tiles):
        mods[0:1, i * HS : (i + 1) * HS] = mod_ref[i : i + 1, :]
        mods[1:2, i * HS : (i + 1) * HS] = 1.0 + mod_ref[tiles + i : tiles + i + 1, :]
    step = 16

    def norm(i, carry):
        piece = lax.rem(place + i, pieces)
        load_x(piece).wait()
        for at in range(0, eighth, step):
            rows = pl.ds(pl.multiple_of(piece * eighth + at, step), step)
            wide = x[rows, :].astype(F32)
            mean = jnp.sum(wide, axis=-1, keepdims=True) * (1.0 / width)
            centred = wide - mean
            var = jnp.sum(centred * centred, axis=-1, keepdims=True) * (1.0 / width)
            adapted[rows, :] = (
                centred * lax.rsqrt(var + EPS) * mods[1:2, :] + mods[0:1, :]
            ).astype(BF16)
        return carry

    def piece_rows(chip, core, c):
        start = (chip * D + core) * eighth + c * chunk
        return pl.ds(pl.multiple_of(start, chunk), chunk)

    def along(hop, c):
        rows = piece_rows(mp, dec, c)
        return pltpu.make_async_remote_copy(
            src_ref=adapted.at[rows] if hop == 2 else far.at[hop - 3, rows],
            dst_ref=far.at[hop - 2, rows],
            send_sem=z_send.at[hop - 2, c],
            recv_sem=z_recv.at[hop - 2, c],
            device_id={"tm": lax.rem(mine + 2, n) if hop == 2 else right},
            device_id_type=MESH,
        )

    def across(hop, j, c, sender):
        rows = piece_rows(sender, dec, c)
        return pltpu.make_async_remote_copy(
            src_ref=far.at[hop - 2, rows],
            dst_ref=far.at[hop - 2, rows],
            send_sem=xy_send.at[hop - 2, j - 1, c],
            recv_sem=xy_recv.at[hop - 2, j - 1, c],
            device_id={"mp": lax.rem(mp + j, M)},
            device_id_type=MESH,
        )

    def to_partner(hop, d, j, c, core):
        rows = piece_rows(lax.rem(mp + M - j, M), core, c)
        return pltpu.make_async_remote_copy(
            src_ref=far.at[hop - 2, rows],
            dst_ref=far.at[hop - 2, rows],
            send_sem=core_send.at[hop - 2, d - 1, j, c],
            recv_sem=core_recv.at[hop - 2, d - 1, j, c],
            device_id={"dec": lax.rem(dec + d, D)},
            device_id_type=MESH,
        )

    def advance(hop, c):
        if hop - 1 > far_hops:
            return

        @pl.when(mine >= hop)
        def _():
            along(hop, c).wait_recv()
            if hop + 1 < n:

                @pl.when(mine + 1 < n)
                def _():
                    along(hop + 1, c).start()

            for j in range(1, M):
                across(hop, j, c, mp).start()
            for d in range(1, D):
                to_partner(hop, d, 0, c, dec).start()

    def collect(hop, c):
        if hop - 1 > far_hops:
            return

        @pl.when(mine >= hop)
        def _():
            for j in range(1, M):
                across(hop, j, c, lax.rem(mp + M - j, M)).wait_recv()
                for d in range(1, D):
                    to_partner(hop, d, j, c, dec).start()

    lax.fori_loop(0, 1, norm, 0)
    pl.semaphore_wait(barrier, len(others) + (M - 1) + (D - 1))
    if far_hops:

        @pl.when(mine + 2 < n)
        def _():
            for c in range(chunks):
                along(2, c).start()

    lax.fori_loop(1, pieces, norm, 0)

    def project(first, count, source, loading):
        out = None
        for part in range(parts):
            if loading:
                for at in range(first, first + count):
                    load_w((1, 2, 0)[at], at, part).wait()
            rows = pl.ds(part * depth, depth)
            piece = jnp.dot(
                source[:, rows],
                w[rows, pl.ds(first * columns, count * columns)],
                preferred_element_type=F32,
            )
            out = piece if out is None else out + piece
        return out.astype(BF16)

    def pass_on(hop, head):
        return pltpu.make_async_remote_copy(
            src_ref=kv.at[hop - 1, head],
            dst_ref=kv.at[hop, head],
            send_sem=kv_send.at[hop - 1, head],
            recv_sem=kv_recv.at[hop - 1, head],
            device_id={"tm": right},
            device_id_type=MESH,
        )

    def keep_kv(slot, block):
        for head in range(heads):
            kv[slot, head, 0] = block[:, head * HS : (head + 1) * HS]
            kv[slot, head, 1] = block[:, columns + head * HS : columns + (head + 1) * HS]

    def send_own(first, last):
        @pl.when(mine + 1 < n)
        def _():
            for head in range(first, last):
                pass_on(1, head).start()

    keep_kv(0, project(0, 2, adapted, True))
    for c in range(chunks - 1):
        advance(2, c)
    send_own(0, 1)
    q[...] = project(2, 1, adapted, True)
    slots = lax.broadcasted_iota(jnp.int32, (1, tok), 1)
    factor = math.log2(math.e) / math.sqrt(HS)

    def scores(hop, head):
        group = mine - hop
        live = jnp.where(mask_ref[mine, group] == 1, len_ref[group], 0)
        score = lax.dot_general(
            q[:, head * HS : (head + 1) * HS],
            kv[hop, head, 0],
            (((1,), (1,)), ((), ())),
            preferred_element_type=F32,
        )
        return jnp.where(slots < live, score * factor, -1e30)

    for head in range(heads):
        score = scores(0, head)
        top = jnp.max(score, axis=-1, keepdims=True)
        weight = jnp.exp2(score - top)
        peak[head] = top
        total[head] = jnp.sum(weight, axis=-1, keepdims=True)
        accum[head] = jnp.dot(
            weight.astype(BF16), kv[0, head, 1], preferred_element_type=F32
        )

    def update(hop, head):
        score = scores(hop, head)
        old = peak[head]
        top = jnp.maximum(old, jnp.max(score, axis=-1, keepdims=True))
        keep = jnp.exp2(old - top)
        weight = jnp.exp2(score - top)
        peak[head] = top
        total[head] = total[head] * keep + jnp.sum(weight, axis=-1, keepdims=True)
        accum[head] = accum[head] * keep + jnp.dot(
            weight.astype(BF16), kv[hop, head, 1], preferred_element_type=F32
        )

    advance(2, chunks - 1)
    send_own(1, heads)
    for c in range(chunks):
        advance(3, c)
        collect(2, c)

    def far_step(hop):
        if hop - 1 > far_hops:
            return

        @pl.when(mine >= hop)
        def _():
            for c in range(chunks):
                for d in range(1, D):
                    core = lax.rem(dec + D - d, D)
                    for j in range(M):
                        to_partner(hop, d, j, c, core).wait_recv()
            keep_kv(hop, project(0, 2, far.at[hop - 2], False))
            for head in range(heads):
                update(hop, head)

    far_step(2)

    def near_step(hop, carry):
        @pl.when(mine >= hop)
        def _():
            for head in range(heads):
                pass_on(hop, head).wait_recv()

                @pl.when((mine + 1 < n) & (hop < near))
                def _():
                    pass_on(hop + 1, head).start()

                update(hop, head)

        return carry

    lax.fori_loop(1, near + 1, near_step, 0)
    for hop in range(3, far_hops + 2):
        if hop > 3:
            for c in range(chunks):
                advance(hop, c)
        for c in range(chunks):
            collect(hop, c)
        far_step(hop)
    for head in range(heads):
        attended[:, head * HS : (head + 1) * HS] = (accum[head] / total[head]).astype(BF16)
    load_wo.wait()

    def term(chip, core):
        start = pl.multiple_of((chip * D + core) * share, share)
        return jnp.dot(attended[...], wo[:, pl.ds(start, share)], preferred_element_type=F32)

    def to_core(d, j):
        return pltpu.make_async_remote_copy(
            src_ref=tx1.at[d - 1, j],
            dst_ref=rx1.at[d - 1, j],
            send_sem=send1.at[d - 1, j],
            recv_sem=recv1.at[d - 1, j],
            device_id={"dec": lax.rem(dec + d, D)},
            device_id_type=MESH,
        )

    def to_chip(j):
        return pltpu.make_async_remote_copy(
            src_ref=tx2.at[j - 1],
            dst_ref=rx2.at[j - 1],
            send_sem=send2.at[j - 1],
            recv_sem=recv2.at[j - 1],
            device_id={"mp": lax.rem(mp + j, M)},
            device_id_type=MESH,
        )

    order = list(range(1, M)) + [0]
    for j in order:
        for d in range(1, D):
            tx1[d - 1, j] = term(lax.rem(mp + j, M), lax.rem(dec + d, D)).astype(BF16)
            to_core(d, j).start()
    for j in order:
        part = term(lax.rem(mp + j, M), dec)
        for d in range(1, D):
            to_core(d, j).wait_recv()
            part = part + rx1[d - 1, j].astype(F32)
        if j > 0:
            tx2[j - 1] = part.astype(BF16)
            to_chip(j).start()
    for j in range(1, M):
        to_chip(j).wait_recv()
        part = part + rx2[j - 1].astype(F32)
    mine_columns = pl.ds(pl.multiple_of((mp * D + dec) * share, share), share)
    first = 2 * tiles + place * (share // HS)
    gate = jnp.concatenate(
        [mod_ref[pl.ds(first + i, 1), :] for i in range(share // HS)], axis=1
    )
    out_ref[...] = (x[:, mine_columns].astype(F32) + gate * part).astype(BF16)

    for j in order:
        for d in range(1, D):
            to_core(d, j).wait_send()
    for j in range(1, M):
        to_chip(j).wait_send()

    def sent(hop, carry):
        @pl.when((mine + 1 < n) & (mine >= hop - 1))
        def _():
            for head in range(heads):
                pass_on(hop, head).wait_send()

        return carry

    lax.fori_loop(1, near + 1, sent, 0)
    for hop in range(2, far_hops + 2):
        reach = mine + 2 < n if hop == 2 else (mine + 1 < n) & (mine >= hop - 1)

        @pl.when(reach)
        def _():
            for c in range(chunks):
                along(hop, c).wait_send()

        @pl.when(mine >= hop)
        def _():
            for c in range(chunks):
                for j in range(1, M):
                    across(hop, j, c, mp).wait_send()
                for j in range(M):
                    for d in range(1, D):
                        to_partner(hop, d, j, c, dec).wait_send()


def solution(mesh):
    n, M, D = mesh.shape["tm"], mesh.shape["mp"], mesh.shape["dec"]

    def shards(latents, modulation, w_qkv, w_out, block_mask, lengths):
        tok, width = latents.shape
        columns = w_qkv.shape[2]
        heads = columns // HS
        share = width // (M * D)
        parts = 3
        chunks = 2
        tiles = width // HS
        far_hops = n - 2 if (n - 2) * tok * width * 2 <= FAR_BYTES else 0
        slots = max(far_hops, 1)
        vmem = pl.BlockSpec(memory_space=pltpu.VMEM)
        smem = pl.BlockSpec(memory_space=pltpu.SMEM)
        anywhere = pl.BlockSpec(memory_space=pl.ANY)
        dma = pltpu.SemaphoreType.DMA
        return pl.pallas_call(
            functools.partial(kernel, (n, M, D, parts, chunks, far_hops)),
            out_shape=jax.ShapeDtypeStruct((tok, share), BF16),
            in_specs=[anywhere, vmem, anywhere, anywhere, smem, smem],
            out_specs=vmem,
            scratch_shapes=[
                pltpu.VMEM((tok, width), BF16),
                pltpu.VMEM((tok, width), BF16),
                pltpu.VMEM((width, 3 * columns), BF16),
                pltpu.VMEM((columns, width), BF16),
                pltpu.VMEM((tok, columns), BF16),
                pltpu.VMEM((n, heads, 2, tok, HS), BF16),
                pltpu.VMEM((heads, tok, 1), F32),
                pltpu.VMEM((heads, tok, 1), F32),
                pltpu.VMEM((heads, tok, HS), F32),
                pltpu.VMEM((tok, columns), BF16),
                pltpu.VMEM((D - 1, M, tok, share), BF16),
                pltpu.VMEM((D - 1, M, tok, share), BF16),
                pltpu.VMEM((M - 1, tok, share), BF16),
                pltpu.VMEM((M - 1, tok, share), BF16),
                pltpu.VMEM((2, width), F32),
                pltpu.VMEM((slots, tok if far_hops else 16, width), BF16),
                dma((M * D,)),
                dma((3, parts)),
                dma,
                dma((n - 1, heads)),
                dma((n - 1, heads)),
                dma((D - 1, M)),
                dma((D - 1, M)),
                dma((M - 1,)),
                dma((M - 1,)),
                dma((slots, chunks)),
                dma((slots, chunks)),
                dma((slots, M - 1, chunks)),
                dma((slots, M - 1, chunks)),
                dma((slots, D - 1, M, chunks)),
                dma((slots, D - 1, M, chunks)),
            ],
            compiler_params=pltpu.CompilerParams(collective_id=0, has_side_effects=True),
        )(latents, modulation.reshape(3 * tiles, HS), w_qkv, w_out, block_mask, lengths)

    return jax.shard_map(
        shards,
        mesh=mesh,
        in_specs=(
            P("tm", None),
            P("tm", None, None),
            P(None, None, ("mp", "dec")),
            P(("mp", "dec"), None),
            P(),
            P(),
        ),
        out_specs=P("tm", ("mp", "dec")),
        check_vma=False,
    )
```

```python
import functools
import math

import jax
import jax.numpy as jnp
from jax import lax
from jax.experimental import pallas as pl
from jax.experimental.pallas import tpu as pltpu
from jax.sharding import PartitionSpec as P

HS = 128
EPS = 1e-6
FAR_BYTES = 16 * 2**20
MESH = pl.DeviceIdType.MESH
F32 = jnp.float32
BF16 = jnp.bfloat16


def kernel(
    sizes,
    lat_hbm,
    mod_ref,
    wqkv_hbm,
    wout_hbm,
    mask_ref,
    len_ref,
    out_ref,
    x,
    adapted,
    w,
    wo,
    q,
    kv,
    peak,
    total,
    accum,
    attended,
    tx1,
    rx1,
    tx2,
    rx2,
    mods,
    far,
    x_sem,
    w_sem,
    wo_sem,
    kv_send,
    kv_recv,
    send1,
    recv1,
    send2,
    recv2,
    z_send,
    z_recv,
    xy_send,
    xy_recv,
    core_send,
    core_recv,
):
    n, M, D, parts, chunks, far_hops = sizes
    near = n - 1 - far_hops
    tok, width = x.shape
    columns = q.shape[1]
    heads = columns // HS
    share = out_ref.shape[1]
    depth = width // parts
    mine = lax.axis_index("tm")
    mp = lax.axis_index("mp")
    dec = lax.axis_index("dec")

    def load_w(which, place, part):
        rows = pl.ds(part * depth, depth)
        return pltpu.make_async_copy(
            wqkv_hbm.at[which, rows],
            w.at[rows, pl.ds(place * columns, columns)],
            w_sem.at[place, part],
        )

    pieces = M * D
    eighth = tok // pieces
    chunk = eighth // chunks
    place = mp * D + dec

    def load_x(i):
        rows = pl.ds(pl.multiple_of(i * eighth, eighth), eighth)
        return pltpu.make_async_copy(lat_hbm.at[rows], x.at[rows], x_sem.at[i])

    load_wo = pltpu.make_async_copy(wout_hbm, wo, wo_sem)
    for i in range(pieces):
        load_x(lax.rem(place + i, pieces)).start()
    for part in range(parts):
        load_w(1, 0, part).start()
        load_w(2, 1, part).start()
    for part in range(parts):
        load_w(0, 2, part).start()
    load_wo.start()

    barrier = pltpu.get_barrier_semaphore()
    right = lax.rem(mine + 1, n)
    left = lax.rem(mine + n - 1, n)
    others = [left, right]
    if far_hops:
        others += [lax.rem(mine + 2, n), lax.rem(mine + n - 2, n)]
    for other in others:
        pl.semaphore_signal(barrier, inc=1, device_id={"tm": other}, device_id_type=MESH)
    for j in range(1, M):
        pl.semaphore_signal(
            barrier, inc=1, device_id={"mp": lax.rem(mp + j, M)}, device_id_type=MESH
        )
    for d in range(1, D):
        pl.semaphore_signal(
            barrier, inc=1, device_id={"dec": lax.rem(dec + d, D)}, device_id_type=MESH
        )

    tiles = width // HS
    for i in range(tiles):
        mods[0:1, i * HS : (i + 1) * HS] = mod_ref[i : i + 1, :]
        mods[1:2, i * HS : (i + 1) * HS] = 1.0 + mod_ref[tiles + i : tiles + i + 1, :]
    step = 16

    def norm(i, carry):
        piece = lax.rem(place + i, pieces)
        load_x(piece).wait()
        for at in range(0, eighth, step):
            rows = pl.ds(pl.multiple_of(piece * eighth + at, step), step)
            wide = x[rows, :].astype(F32)
            mean = jnp.sum(wide, axis=-1, keepdims=True) * (1.0 / width)
            centred = wide - mean
            var = jnp.sum(centred * centred, axis=-1, keepdims=True) * (1.0 / width)
            adapted[rows, :] = (
                centred * lax.rsqrt(var + EPS) * mods[1:2, :] + mods[0:1, :]
            ).astype(BF16)
        return carry

    def piece_rows(chip, core, c):
        start = (chip * D + core) * eighth + c * chunk
        return pl.ds(pl.multiple_of(start, chunk), chunk)

    def along(hop, c):
        rows = piece_rows(mp, dec, c)
        return pltpu.make_async_remote_copy(
            src_ref=adapted.at[rows] if hop == 2 else far.at[hop - 3, rows],
            dst_ref=far.at[hop - 2, rows],
            send_sem=z_send.at[hop - 2, c],
            recv_sem=z_recv.at[hop - 2, c],
            device_id={"tm": lax.rem(mine + 2, n) if hop == 2 else right},
            device_id_type=MESH,
        )

    x_chip = mp + 1 - 2 * lax.rem(mp, 2)
    y_chip = lax.rem(mp + 2, M)
    chips = (mp, x_chip, y_chip, lax.rem(x_chip + 2, M))

    def across(hop, j, c, origin):
        rows = piece_rows(chips[origin], dec, c)
        along_x = j == 1 or (j == 3 and c % 2 == 1)
        return pltpu.make_async_remote_copy(
            src_ref=far.at[hop - 2, rows],
            dst_ref=far.at[hop - 2, rows],
            send_sem=xy_send.at[hop - 2, j - 1, c],
            recv_sem=xy_recv.at[hop - 2, j - 1, c],
            device_id={"mp": x_chip if along_x else y_chip},
            device_id_type=MESH,
        )

    def to_partner(hop, d, j, c, core):
        rows = piece_rows(chips[j], core, c)
        return pltpu.make_async_remote_copy(
            src_ref=far.at[hop - 2, rows],
            dst_ref=far.at[hop - 2, rows],
            send_sem=core_send.at[hop - 2, d - 1, j, c],
            recv_sem=core_recv.at[hop - 2, d - 1, j, c],
            device_id={"dec": lax.rem(dec + d, D)},
            device_id_type=MESH,
        )

    def advance(hop, c):
        if hop - 1 > far_hops:
            return

        @pl.when(mine >= hop)
        def _():
            along(hop, c).wait_recv()
            if hop + 1 < n:

                @pl.when(mine + 1 < n)
                def _():
                    along(hop + 1, c).start()

            for j in (1, 2):
                across(hop, j, c, 0).start()
            for d in range(1, D):
                to_partner(hop, d, 0, c, dec).start()

    def via(c):
        return 1 + c % 2

    def relay(hop):
        if hop - 1 > far_hops:
            return

        @pl.when(mine >= hop)
        def _():
            for c in range(chunks):
                across(hop, via(c), c, via(c)).wait_recv()
                across(hop, 3, c, via(c)).start()
                for d in range(1, D):
                    to_partner(hop, d, via(c), c, dec).start()

    def collect(hop):
        if hop - 1 > far_hops:
            return

        @pl.when(mine >= hop)
        def _():
            for c in range(chunks):
                for j in (3 - via(c), 3):
                    across(hop, j, c, j).wait_recv()
                    for d in range(1, D):
                        to_partner(hop, d, j, c, dec).start()

    lax.fori_loop(0, 1, norm, 0)
    pl.semaphore_wait(barrier, len(others) + (M - 1) + (D - 1))
    if far_hops:

        @pl.when(mine + 2 < n)
        def _():
            for c in range(chunks):
                along(2, c).start()

    lax.fori_loop(1, pieces, norm, 0)

    def project(first, count, source, loading):
        out = None
        for part in range(parts):
            if loading:
                for at in range(first, first + count):
                    load_w((1, 2, 0)[at], at, part).wait()
            rows = pl.ds(part * depth, depth)
            piece = jnp.dot(
                source[:, rows],
                w[rows, pl.ds(first * columns, count * columns)],
                preferred_element_type=F32,
            )
            out = piece if out is None else out + piece
        return out.astype(BF16)

    def pass_on(hop, head):
        return pltpu.make_async_remote_copy(
            src_ref=kv.at[hop - 1, head],
            dst_ref=kv.at[hop, head],
            send_sem=kv_send.at[hop - 1, head],
            recv_sem=kv_recv.at[hop - 1, head],
            device_id={"tm": right},
            device_id_type=MESH,
        )

    def keep_kv(slot, block):
        for head in range(heads):
            kv[slot, head, 0] = block[:, head * HS : (head + 1) * HS]
            kv[slot, head, 1] = block[:, columns + head * HS : columns + (head + 1) * HS]

    def send_own(first, last):
        @pl.when(mine + 1 < n)
        def _():
            for head in range(first, last):
                pass_on(1, head).start()

    keep_kv(0, project(0, 2, adapted, True))
    for c in range(chunks - 1):
        advance(2, c)
    send_own(0, 1)
    q[...] = project(2, 1, adapted, True)
    slots = lax.broadcasted_iota(jnp.int32, (1, tok), 1)
    factor = math.log2(math.e) / math.sqrt(HS)

    def scores(hop, head):
        group = mine - hop
        live = jnp.where(mask_ref[mine, group] == 1, len_ref[group], 0)
        score = lax.dot_general(
            q[:, head * HS : (head + 1) * HS],
            kv[hop, head, 0],
            (((1,), (1,)), ((), ())),
            preferred_element_type=F32,
        )
        return jnp.where(slots < live, score * factor, -1e30)

    for head in range(heads):
        score = scores(0, head)
        top = jnp.max(score, axis=-1, keepdims=True)
        weight = jnp.exp2(score - top)
        peak[head] = top
        total[head] = jnp.sum(weight, axis=-1, keepdims=True)
        accum[head] = jnp.dot(
            weight.astype(BF16), kv[0, head, 1], preferred_element_type=F32
        )

    def update(hop, head):
        score = scores(hop, head)
        old = peak[head]
        top = jnp.maximum(old, jnp.max(score, axis=-1, keepdims=True))
        keep = jnp.exp2(old - top)
        weight = jnp.exp2(score - top)
        peak[head] = top
        total[head] = total[head] * keep + jnp.sum(weight, axis=-1, keepdims=True)
        accum[head] = accum[head] * keep + jnp.dot(
            weight.astype(BF16), kv[hop, head, 1], preferred_element_type=F32
        )

    advance(2, chunks - 1)
    send_own(1, heads)
    relay(2)
    for c in range(chunks):
        advance(3, c)
    collect(2)

    def far_step(hop):
        if hop - 1 > far_hops:
            return

        @pl.when(mine >= hop)
        def _():
            for c in range(chunks):
                for d in range(1, D):
                    core = lax.rem(dec + D - d, D)
                    for j in range(M):
                        to_partner(hop, d, j, c, core).wait_recv()
            keep_kv(hop, project(0, 2, far.at[hop - 2], False))
            for head in range(heads):
                update(hop, head)

    far_step(2)
    relay(3)

    def near_step(hop, carry):
        @pl.when(mine >= hop)
        def _():
            for head in range(heads):
                pass_on(hop, head).wait_recv()

                @pl.when((mine + 1 < n) & (hop < near))
                def _():
                    pass_on(hop + 1, head).start()

                update(hop, head)

        return carry

    lax.fori_loop(1, near + 1, near_step, 0)
    for hop in range(3, far_hops + 2):
        if hop > 3:
            for c in range(chunks):
                advance(hop, c)
            relay(hop)
        collect(hop)
        far_step(hop)
    for head in range(heads):
        attended[:, head * HS : (head + 1) * HS] = (accum[head] / total[head]).astype(BF16)
    load_wo.wait()

    def term(chip, core):
        start = pl.multiple_of((chip * D + core) * share, share)
        return jnp.dot(attended[...], wo[:, pl.ds(start, share)], preferred_element_type=F32)

    def to_core(d, j):
        return pltpu.make_async_remote_copy(
            src_ref=tx1.at[d - 1, j],
            dst_ref=rx1.at[d - 1, j],
            send_sem=send1.at[d - 1, j],
            recv_sem=recv1.at[d - 1, j],
            device_id={"dec": lax.rem(dec + d, D)},
            device_id_type=MESH,
        )

    def to_chip(j):
        return pltpu.make_async_remote_copy(
            src_ref=tx2.at[j - 1],
            dst_ref=rx2.at[j - 1],
            send_sem=send2.at[j - 1],
            recv_sem=recv2.at[j - 1],
            device_id={"mp": lax.rem(mp + j, M)},
            device_id_type=MESH,
        )

    order = list(range(1, M)) + [0]
    for j in order:
        for d in range(1, D):
            tx1[d - 1, j] = term(lax.rem(mp + j, M), lax.rem(dec + d, D)).astype(BF16)
            to_core(d, j).start()
    for j in order:
        part = term(lax.rem(mp + j, M), dec)
        for d in range(1, D):
            to_core(d, j).wait_recv()
            part = part + rx1[d - 1, j].astype(F32)
        if j > 0:
            tx2[j - 1] = part.astype(BF16)
            to_chip(j).start()
    for j in range(1, M):
        to_chip(j).wait_recv()
        part = part + rx2[j - 1].astype(F32)
    mine_columns = pl.ds(pl.multiple_of((mp * D + dec) * share, share), share)
    first = 2 * tiles + place * (share // HS)
    gate = jnp.concatenate(
        [mod_ref[pl.ds(first + i, 1), :] for i in range(share // HS)], axis=1
    )
    out_ref[...] = (x[:, mine_columns].astype(F32) + gate * part).astype(BF16)

    for j in order:
        for d in range(1, D):
            to_core(d, j).wait_send()
    for j in range(1, M):
        to_chip(j).wait_send()

    def sent(hop, carry):
        @pl.when((mine + 1 < n) & (mine >= hop - 1))
        def _():
            for head in range(heads):
                pass_on(hop, head).wait_send()

        return carry

    lax.fori_loop(1, near + 1, sent, 0)
    for hop in range(2, far_hops + 2):
        reach = mine + 2 < n if hop == 2 else (mine + 1 < n) & (mine >= hop - 1)

        @pl.when(reach)
        def _():
            for c in range(chunks):
                along(hop, c).wait_send()

        @pl.when(mine >= hop)
        def _():
            for c in range(chunks):
                for j in (1, 2):
                    across(hop, j, c, 0).wait_send()
                across(hop, 3, c, via(c)).wait_send()
                for j in range(M):
                    for d in range(1, D):
                        to_partner(hop, d, j, c, dec).wait_send()


def solution(mesh):
    n, M, D = mesh.shape["tm"], mesh.shape["mp"], mesh.shape["dec"]

    def shards(latents, modulation, w_qkv, w_out, block_mask, lengths):
        tok, width = latents.shape
        columns = w_qkv.shape[2]
        heads = columns // HS
        share = width // (M * D)
        parts = 3
        chunks = 2
        tiles = width // HS
        far_hops = n - 2 if M == 4 and (n - 2) * tok * width * 2 <= FAR_BYTES else 0
        slots = max(far_hops, 1)
        vmem = pl.BlockSpec(memory_space=pltpu.VMEM)
        smem = pl.BlockSpec(memory_space=pltpu.SMEM)
        anywhere = pl.BlockSpec(memory_space=pl.ANY)
        dma = pltpu.SemaphoreType.DMA
        return pl.pallas_call(
            functools.partial(kernel, (n, M, D, parts, chunks, far_hops)),
            out_shape=jax.ShapeDtypeStruct((tok, share), BF16),
            in_specs=[anywhere, vmem, anywhere, anywhere, smem, smem],
            out_specs=vmem,
            scratch_shapes=[
                pltpu.VMEM((tok, width), BF16),
                pltpu.VMEM((tok, width), BF16),
                pltpu.VMEM((width, 3 * columns), BF16),
                pltpu.VMEM((columns, width), BF16),
                pltpu.VMEM((tok, columns), BF16),
                pltpu.VMEM((n, heads, 2, tok, HS), BF16),
                pltpu.VMEM((heads, tok, 1), F32),
                pltpu.VMEM((heads, tok, 1), F32),
                pltpu.VMEM((heads, tok, HS), F32),
                pltpu.VMEM((tok, columns), BF16),
                pltpu.VMEM((D - 1, M, tok, share), BF16),
                pltpu.VMEM((D - 1, M, tok, share), BF16),
                pltpu.VMEM((M - 1, tok, share), BF16),
                pltpu.VMEM((M - 1, tok, share), BF16),
                pltpu.VMEM((2, width), F32),
                pltpu.VMEM((slots, tok if far_hops else 16, width), BF16),
                dma((M * D,)),
                dma((3, parts)),
                dma,
                dma((n - 1, heads)),
                dma((n - 1, heads)),
                dma((D - 1, M)),
                dma((D - 1, M)),
                dma((M - 1,)),
                dma((M - 1,)),
                dma((slots, chunks)),
                dma((slots, chunks)),
                dma((slots, M - 1, chunks)),
                dma((slots, M - 1, chunks)),
                dma((slots, D - 1, M, chunks)),
                dma((slots, D - 1, M, chunks)),
            ],
            compiler_params=pltpu.CompilerParams(collective_id=0, has_side_effects=True),
        )(latents, modulation.reshape(3 * tiles, HS), w_qkv, w_out, block_mask, lengths)

    return jax.shard_map(
        shards,
        mesh=mesh,
        in_specs=(
            P("tm", None),
            P("tm", None, None),
            P(None, None, ("mp", "dec")),
            P(("mp", "dec"), None),
            P(),
            P(),
        ),
        out_specs=P("tm", ("mp", "dec")),
        check_vma=False,
    )
```

```python
import functools
import math

import jax
import jax.numpy as jnp
from jax import lax
from jax.experimental import pallas as pl
from jax.experimental.pallas import tpu as pltpu
from jax.sharding import PartitionSpec as P

HS = 128
EPS = 1e-6
FAR_BYTES = 16 * 2**20
MESH = pl.DeviceIdType.MESH
F32 = jnp.float32
BF16 = jnp.bfloat16


def kernel(
    sizes,
    lat_hbm,
    mod_ref,
    wqkv_hbm,
    wout_hbm,
    mask_ref,
    len_ref,
    out_ref,
    x,
    adapted,
    w,
    wo,
    q,
    kv,
    peak,
    total,
    accum,
    attended,
    tx1,
    rx1,
    tx2,
    rx2,
    mods,
    far,
    x_sem,
    w_sem,
    wo_sem,
    kv_send,
    kv_recv,
    send1,
    recv1,
    send2,
    recv2,
    z_send,
    z_recv,
    xy_send,
    xy_recv,
    core_send,
    core_recv,
):
    n, M, D, parts, chunks, far_hops = sizes
    near = n - 1 - far_hops
    tok, width = x.shape
    columns = q.shape[1]
    heads = columns // HS
    share = out_ref.shape[1]
    depth = width // parts
    mine = lax.axis_index("tm")
    mp = lax.axis_index("mp")
    dec = lax.axis_index("dec")

    def load_w(which, place, part):
        rows = pl.ds(part * depth, depth)
        return pltpu.make_async_copy(
            wqkv_hbm.at[which, rows],
            w.at[rows, pl.ds(place * columns, columns)],
            w_sem.at[place, part],
        )

    pieces = M * D
    eighth = tok // pieces
    chunk = eighth // chunks
    place = mp * D + dec

    def load_x(i):
        rows = pl.ds(pl.multiple_of(i * eighth, eighth), eighth)
        return pltpu.make_async_copy(lat_hbm.at[rows], x.at[rows], x_sem.at[i])

    load_wo = pltpu.make_async_copy(wout_hbm, wo, wo_sem)
    for i in range(pieces):
        load_x(lax.rem(place + i, pieces)).start()

    barrier = pltpu.get_barrier_semaphore()
    right = lax.rem(mine + 1, n)
    left = lax.rem(mine + n - 1, n)
    others = [left, right]
    if far_hops:
        others += [lax.rem(mine + 2, n), lax.rem(mine + n - 2, n)]
    for other in others:
        pl.semaphore_signal(barrier, inc=1, device_id={"tm": other}, device_id_type=MESH)
    for j in range(1, M):
        pl.semaphore_signal(
            barrier, inc=1, device_id={"mp": lax.rem(mp + j, M)}, device_id_type=MESH
        )
    for d in range(1, D):
        pl.semaphore_signal(
            barrier, inc=1, device_id={"dec": lax.rem(dec + d, D)}, device_id_type=MESH
        )

    tiles = width // HS
    for i in range(tiles):
        mods[0:1, i * HS : (i + 1) * HS] = mod_ref[i : i + 1, :]
        mods[1:2, i * HS : (i + 1) * HS] = 1.0 + mod_ref[tiles + i : tiles + i + 1, :]
    step = 16

    def norm(i, carry):
        piece = lax.rem(place + i, pieces)
        load_x(piece).wait()
        for at in range(0, eighth, step):
            rows = pl.ds(pl.multiple_of(piece * eighth + at, step), step)
            wide = x[rows, :].astype(F32)
            mean = jnp.sum(wide, axis=-1, keepdims=True) * (1.0 / width)
            centred = wide - mean
            var = jnp.sum(centred * centred, axis=-1, keepdims=True) * (1.0 / width)
            adapted[rows, :] = (
                centred * lax.rsqrt(var + EPS) * mods[1:2, :] + mods[0:1, :]
            ).astype(BF16)
        return carry

    def piece_rows(chip, core, c):
        start = (chip * D + core) * eighth + c * chunk
        return pl.ds(pl.multiple_of(start, chunk), chunk)

    def along(hop, c):
        rows = piece_rows(mp, dec, c)
        return pltpu.make_async_remote_copy(
            src_ref=adapted.at[rows] if hop == 2 else far.at[hop - 3, rows],
            dst_ref=far.at[hop - 2, rows],
            send_sem=z_send.at[hop - 2, c],
            recv_sem=z_recv.at[hop - 2, c],
            device_id={"tm": lax.rem(mine + 2, n) if hop == 2 else right},
            device_id_type=MESH,
        )

    x_chip = mp + 1 - 2 * lax.rem(mp, 2)
    y_chip = lax.rem(mp + 2, M)
    chips = (mp, x_chip, y_chip, lax.rem(x_chip + 2, M))

    def across(hop, j, c, origin):
        rows = piece_rows(chips[origin], dec, c)
        along_x = j == 1 or (j == 3 and c % 2 == 1)
        return pltpu.make_async_remote_copy(
            src_ref=far.at[hop - 2, rows],
            dst_ref=far.at[hop - 2, rows],
            send_sem=xy_send.at[hop - 2, j - 1, c],
            recv_sem=xy_recv.at[hop - 2, j - 1, c],
            device_id={"mp": x_chip if along_x else y_chip},
            device_id_type=MESH,
        )

    def to_partner(hop, d, j, c, core):
        rows = piece_rows(chips[j], core, c)
        return pltpu.make_async_remote_copy(
            src_ref=far.at[hop - 2, rows],
            dst_ref=far.at[hop - 2, rows],
            send_sem=core_send.at[hop - 2, d - 1, j, c],
            recv_sem=core_recv.at[hop - 2, d - 1, j, c],
            device_id={"dec": lax.rem(dec + d, D)},
            device_id_type=MESH,
        )

    def advance(hop, c):
        if hop - 1 > far_hops:
            return

        @pl.when(mine >= hop)
        def _():
            along(hop, c).wait_recv()
            if hop + 1 < n:

                @pl.when(mine + 1 < n)
                def _():
                    along(hop + 1, c).start()

            for j in (1, 2):
                across(hop, j, c, 0).start()
            for d in range(1, D):
                to_partner(hop, d, 0, c, dec).start()

    def via(c):
        return 1 + c % 2

    def relay(hop):
        if hop - 1 > far_hops:
            return

        @pl.when(mine >= hop)
        def _():
            for c in range(chunks):
                across(hop, via(c), c, via(c)).wait_recv()
                across(hop, 3, c, via(c)).start()
                for d in range(1, D):
                    to_partner(hop, d, via(c), c, dec).start()

    def collect(hop):
        if hop - 1 > far_hops:
            return

        @pl.when(mine >= hop)
        def _():
            for c in range(chunks):
                for j in (3 - via(c), 3):
                    across(hop, j, c, j).wait_recv()
                    for d in range(1, D):
                        to_partner(hop, d, j, c, dec).start()

    lax.fori_loop(0, 1, norm, 0)
    pl.semaphore_wait(barrier, len(others) + (M - 1) + (D - 1))

    def start_far(which):
        @pl.when(which & (mine + 2 < n))
        def _():
            for c in range(chunks):
                along(2, c).start()

    if far_hops:
        start_far(mine == 0)
    for part in range(parts):
        load_w(1, 0, part).start()
        load_w(2, 1, part).start()
    for part in range(parts):
        load_w(0, 2, part).start()
    load_wo.start()
    lax.fori_loop(1, pieces, norm, 0)
    if far_hops:
        start_far(mine > 0)

    def project(first, count, source, loading):
        out = None
        for part in range(parts):
            if loading:
                for at in range(first, first + count):
                    load_w((1, 2, 0)[at], at, part).wait()
            rows = pl.ds(part * depth, depth)
            piece = jnp.dot(
                source[:, rows],
                w[rows, pl.ds(first * columns, count * columns)],
                preferred_element_type=F32,
            )
            out = piece if out is None else out + piece
        return out.astype(BF16)

    def pass_on(hop, head):
        return pltpu.make_async_remote_copy(
            src_ref=kv.at[hop - 1, head],
            dst_ref=kv.at[hop, head],
            send_sem=kv_send.at[hop - 1, head],
            recv_sem=kv_recv.at[hop - 1, head],
            device_id={"tm": right},
            device_id_type=MESH,
        )

    def keep_kv(slot, block):
        for head in range(heads):
            kv[slot, head, 0] = block[:, head * HS : (head + 1) * HS]
            kv[slot, head, 1] = block[:, columns + head * HS : columns + (head + 1) * HS]

    def send_own(first, last):
        @pl.when(mine + 1 < n)
        def _():
            for head in range(first, last):
                pass_on(1, head).start()

    keep_kv(0, project(0, 2, adapted, True))
    for c in range(chunks - 1):
        advance(2, c)
    send_own(0, 1)
    q[...] = project(2, 1, adapted, True)
    advance(2, chunks - 1)
    send_own(1, heads)
    for c in range(chunks):
        advance(3, c)
    slots = lax.broadcasted_iota(jnp.int32, (1, tok), 1)
    factor = math.log2(math.e) / math.sqrt(HS)

    def scores(hop, head):
        group = mine - hop
        live = jnp.where(mask_ref[mine, group] == 1, len_ref[group], 0)
        score = lax.dot_general(
            q[:, head * HS : (head + 1) * HS],
            kv[hop, head, 0],
            (((1,), (1,)), ((), ())),
            preferred_element_type=F32,
        )
        return jnp.where(slots < live, score * factor, -1e30)

    for head in range(heads):
        score = scores(0, head)
        top = jnp.max(score, axis=-1, keepdims=True)
        weight = jnp.exp2(score - top)
        peak[head] = top
        total[head] = jnp.sum(weight, axis=-1, keepdims=True)
        accum[head] = jnp.dot(
            weight.astype(BF16), kv[0, head, 1], preferred_element_type=F32
        )

    def update(hop, head):
        score = scores(hop, head)
        old = peak[head]
        top = jnp.maximum(old, jnp.max(score, axis=-1, keepdims=True))
        keep = jnp.exp2(old - top)
        weight = jnp.exp2(score - top)
        peak[head] = top
        total[head] = total[head] * keep + jnp.sum(weight, axis=-1, keepdims=True)
        accum[head] = accum[head] * keep + jnp.dot(
            weight.astype(BF16), kv[hop, head, 1], preferred_element_type=F32
        )

    relay(2)
    relay(3)
    collect(2)

    def far_step(hop):
        if hop - 1 > far_hops:
            return

        @pl.when(mine >= hop)
        def _():
            for c in range(chunks):
                for d in range(1, D):
                    core = lax.rem(dec + D - d, D)
                    for j in range(M):
                        to_partner(hop, d, j, c, core).wait_recv()
            keep_kv(hop, project(0, 2, far.at[hop - 2], False))
            for head in range(heads):
                update(hop, head)

    far_step(2)

    def near_step(hop, carry):
        @pl.when(mine >= hop)
        def _():
            for head in range(heads):
                pass_on(hop, head).wait_recv()

                @pl.when((mine + 1 < n) & (hop < near))
                def _():
                    pass_on(hop + 1, head).start()

                update(hop, head)

        return carry

    lax.fori_loop(1, near + 1, near_step, 0)
    for hop in range(3, far_hops + 2):
        if hop > 3:
            for c in range(chunks):
                advance(hop, c)
            relay(hop)
        collect(hop)
        far_step(hop)
    for head in range(heads):
        attended[:, head * HS : (head + 1) * HS] = (accum[head] / total[head]).astype(BF16)
    load_wo.wait()

    def term(chip, core):
        start = pl.multiple_of((chip * D + core) * share, share)
        return jnp.dot(attended[...], wo[:, pl.ds(start, share)], preferred_element_type=F32)

    def to_core(d, j):
        return pltpu.make_async_remote_copy(
            src_ref=tx1.at[d - 1, j],
            dst_ref=rx1.at[d - 1, j],
            send_sem=send1.at[d - 1, j],
            recv_sem=recv1.at[d - 1, j],
            device_id={"dec": lax.rem(dec + d, D)},
            device_id_type=MESH,
        )

    def to_chip(j):
        return pltpu.make_async_remote_copy(
            src_ref=tx2.at[j - 1],
            dst_ref=rx2.at[j - 1],
            send_sem=send2.at[j - 1],
            recv_sem=recv2.at[j - 1],
            device_id={"mp": lax.rem(mp + j, M)},
            device_id_type=MESH,
        )

    order = list(range(1, M)) + [0]
    for j in order:
        for d in range(1, D):
            tx1[d - 1, j] = term(lax.rem(mp + j, M), lax.rem(dec + d, D)).astype(BF16)
            to_core(d, j).start()
    for j in order:
        part = term(lax.rem(mp + j, M), dec)
        for d in range(1, D):
            to_core(d, j).wait_recv()
            part = part + rx1[d - 1, j].astype(F32)
        if j > 0:
            tx2[j - 1] = part.astype(BF16)
            to_chip(j).start()
    for j in range(1, M):
        to_chip(j).wait_recv()
        part = part + rx2[j - 1].astype(F32)
    mine_columns = pl.ds(pl.multiple_of((mp * D + dec) * share, share), share)
    first = 2 * tiles + place * (share // HS)
    gate = jnp.concatenate(
        [mod_ref[pl.ds(first + i, 1), :] for i in range(share // HS)], axis=1
    )
    out_ref[...] = (x[:, mine_columns].astype(F32) + gate * part).astype(BF16)

    for j in order:
        for d in range(1, D):
            to_core(d, j).wait_send()
    for j in range(1, M):
        to_chip(j).wait_send()

    def sent(hop, carry):
        @pl.when((mine + 1 < n) & (mine >= hop - 1))
        def _():
            for head in range(heads):
                pass_on(hop, head).wait_send()

        return carry

    lax.fori_loop(1, near + 1, sent, 0)
    for hop in range(2, far_hops + 2):
        reach = mine + 2 < n if hop == 2 else (mine + 1 < n) & (mine >= hop - 1)

        @pl.when(reach)
        def _():
            for c in range(chunks):
                along(hop, c).wait_send()

        @pl.when(mine >= hop)
        def _():
            for c in range(chunks):
                for j in (1, 2):
                    across(hop, j, c, 0).wait_send()
                across(hop, 3, c, via(c)).wait_send()
                for j in range(M):
                    for d in range(1, D):
                        to_partner(hop, d, j, c, dec).wait_send()


def solution(mesh):
    n, M, D = mesh.shape["tm"], mesh.shape["mp"], mesh.shape["dec"]

    def shards(latents, modulation, w_qkv, w_out, block_mask, lengths):
        tok, width = latents.shape
        columns = w_qkv.shape[2]
        heads = columns // HS
        share = width // (M * D)
        parts = 3
        chunks = 2
        tiles = width // HS
        far_hops = n - 2 if M == 4 and (n - 2) * tok * width * 2 <= FAR_BYTES else 0
        slots = max(far_hops, 1)
        vmem = pl.BlockSpec(memory_space=pltpu.VMEM)
        smem = pl.BlockSpec(memory_space=pltpu.SMEM)
        anywhere = pl.BlockSpec(memory_space=pl.ANY)
        dma = pltpu.SemaphoreType.DMA
        return pl.pallas_call(
            functools.partial(kernel, (n, M, D, parts, chunks, far_hops)),
            out_shape=jax.ShapeDtypeStruct((tok, share), BF16),
            in_specs=[anywhere, vmem, anywhere, anywhere, smem, smem],
            out_specs=vmem,
            scratch_shapes=[
                pltpu.VMEM((tok, width), BF16),
                pltpu.VMEM((tok, width), BF16),
                pltpu.VMEM((width, 3 * columns), BF16),
                pltpu.VMEM((columns, width), BF16),
                pltpu.VMEM((tok, columns), BF16),
                pltpu.VMEM((n, heads, 2, tok, HS), BF16),
                pltpu.VMEM((heads, tok, 1), F32),
                pltpu.VMEM((heads, tok, 1), F32),
                pltpu.VMEM((heads, tok, HS), F32),
                pltpu.VMEM((tok, columns), BF16),
                pltpu.VMEM((D - 1, M, tok, share), BF16),
                pltpu.VMEM((D - 1, M, tok, share), BF16),
                pltpu.VMEM((M - 1, tok, share), BF16),
                pltpu.VMEM((M - 1, tok, share), BF16),
                pltpu.VMEM((2, width), F32),
                pltpu.VMEM((slots, tok if far_hops else 16, width), BF16),
                dma((M * D,)),
                dma((3, parts)),
                dma,
                dma((n - 1, heads)),
                dma((n - 1, heads)),
                dma((D - 1, M)),
                dma((D - 1, M)),
                dma((M - 1,)),
                dma((M - 1,)),
                dma((slots, chunks)),
                dma((slots, chunks)),
                dma((slots, M - 1, chunks)),
                dma((slots, M - 1, chunks)),
                dma((slots, D - 1, M, chunks)),
                dma((slots, D - 1, M, chunks)),
            ],
            compiler_params=pltpu.CompilerParams(collective_id=0, has_side_effects=True),
        )(latents, modulation.reshape(3 * tiles, HS), w_qkv, w_out, block_mask, lengths)

    return jax.shard_map(
        shards,
        mesh=mesh,
        in_specs=(
            P("tm", None),
            P("tm", None, None),
            P(None, None, ("mp", "dec")),
            P(("mp", "dec"), None),
            P(),
            P(),
        ),
        out_specs=P("tm", ("mp", "dec")),
        check_vma=False,
    )
```
